8 devices in a mesh: dep: 2 (over z, y), col: 2 (over x), row: 2 (over core).
Axes of the slice: x: 2, y: 2, z: 1, core: 2. Of those that a mesh axis runs over, the one named last changes fastest.
Arguments:
- x_tok: bfloat16 [16384, 1024], P(('dep', 'row'), 'col')
- w_up: bfloat16 [1024, 4096], P('row', 'col')
- w_down: bfloat16 [4096, 1024], P('row', 'col')
- grad_out: bfloat16 [16384, 1024], P(('dep', 'row'), 'col')
Outputs:
- output 1: bfloat16 [16384, 1024], P(('dep', 'row'), 'col')
- output 2: bfloat16 [16384, 1024], P(('dep', 'row'), 'col')
- output 3: float32 [1024, 4096], P(('row', 'dep'), 'col')
- output 4: float32 [4096, 1024], P(('row', 'dep'), 'col')
All inputs are finite; a program needn't handle non-finite values.
Results may differ from the reference program's by a relative error of at most 0.001.
Values are sent between devices in bfloat16 or wider.
A program may use at most 1 GiB of HBM per device.

```python
import math
import jax
import jax.numpy as jnp
from jax import lax

HIDDEN = 1024
FFN_DIM = 4096
TOKENS = 16384

BLOCK_ROWS = math.gcd(TOKENS, 2048)
NUM_BLOCKS = TOKENS // BLOCK_ROWS
GELU_COEF = 0.7978845608028654
CUBIC_COEF = 0.044715


def gelu_fwd(pre_act):
    inner = GELU_COEF * (pre_act + CUBIC_COEF * pre_act * pre_act * pre_act)
    return 0.5 * pre_act * (1.0 + jnp.tanh(inner))


def gelu_slope(pre_act):
    inner = GELU_COEF * (pre_act + CUBIC_COEF * pre_act * pre_act * pre_act)
    tanh_val = jnp.tanh(inner)
    return 0.5 * (1.0 + tanh_val) + 0.5 * pre_act * (1.0 - tanh_val * tanh_val) * GELU_COEF * (1.0 + 3.0 * CUBIC_COEF * pre_act * pre_act)


def setup_inputs(seed: int = 0) -> dict:
    root_key = jax.random.key(seed)
    key_x, key_up, key_down, key_g = jax.random.split(root_key, 4)
    x_tok = jax.random.normal(key_x, (TOKENS, HIDDEN), jnp.float32).astype(jnp.bfloat16)
    w_up = (jax.random.normal(key_up, (HIDDEN, FFN_DIM), jnp.float32) * HIDDEN ** -0.5).astype(jnp.bfloat16)
    w_down = (jax.random.normal(key_down, (FFN_DIM, HIDDEN), jnp.float32) * FFN_DIM ** -0.5).astype(jnp.bfloat16)
    grad_out = jax.random.normal(key_g, (TOKENS, HIDDEN), jnp.float32).astype(jnp.bfloat16)
    return {"x_tok": x_tok, "w_up": w_up, "w_down": w_down, "grad_out": grad_out}


def reference(x_tok, w_up, w_down, grad_out):
    x_blocks = x_tok.reshape(NUM_BLOCKS, BLOCK_ROWS, HIDDEN)
    g_blocks = grad_out.reshape(NUM_BLOCKS, BLOCK_ROWS, HIDDEN)

    def block_step(acc_pair, block_in):
        dw_up_acc, dw_down_acc = acc_pair
        x_blk, g_blk = block_in
        pre_act = jnp.dot(x_blk, w_up, preferred_element_type=jnp.float32)
        hidden_act = gelu_fwd(pre_act).astype(jnp.bfloat16)
        y_blk = jnp.dot(hidden_act, w_down, preferred_element_type=jnp.float32).astype(jnp.bfloat16)
        d_act = jnp.dot(g_blk, w_down.T, preferred_element_type=jnp.float32)
        d_pre = (d_act * gelu_slope(pre_act)).astype(jnp.bfloat16)
        dx_blk = jnp.dot(d_pre, w_up.T, preferred_element_type=jnp.float32).astype(jnp.bfloat16)
        dw_up_acc = dw_up_acc + jnp.dot(x_blk.T, d_pre, preferred_element_type=jnp.float32)
        dw_down_acc = dw_down_acc + jnp.dot(hidden_act.T, g_blk, preferred_element_type=jnp.float32)
        return (dw_up_acc, dw_down_acc), (y_blk, dx_blk)

    init_acc = (jnp.zeros((HIDDEN, FFN_DIM), jnp.float32), jnp.zeros((FFN_DIM, HIDDEN), jnp.float32))
    (dw_up, dw_down), (y_blocks, dx_blocks) = lax.scan(block_step, init_acc, (x_blocks, g_blocks))
    return y_blocks.reshape(TOKENS, HIDDEN), dx_blocks.reshape(TOKENS, HIDDEN), dw_up, dw_down
```

```python
import functools

import jax
import jax.numpy as jnp
from jax import lax
from jax.experimental import pallas as pl
from jax.experimental.pallas import tpu as pltpu
from jax.sharding import PartitionSpec as P

GELU_COEF = 0.7978845608028654
CUBIC_COEF = 0.044715
MESH = pl.DeviceIdType.MESH
F32, BF16 = jnp.float32, jnp.bfloat16
CHUNKS = 8
BLOCKS = 8
RING = 4
AHEAD = 4


def gelu_and_slope(u):
    u2 = u * u
    p = GELU_COEF * CUBIC_COEF * u2 + GELU_COEF
    s = 0.5 * jnp.tanh(u * p) + 0.5
    a = u * s
    return a, s + (a * (1.0 - s)) * (6.0 * GELU_COEF * CUBIC_COEF * u2 + 2.0 * GELU_COEF)


def dot(a, b, ca=1, cb=0):
    return lax.dot_general(a, b, (((ca,), (cb,)), ((), ())), preferred_element_type=F32)


def kernel(x_hbm, w1_hbm, w2_hbm, g_hbm, y_hbm, dx_hbm, dw1_own, dw1_got, dw2_own, dw2_got, slope_hbm,
           w1, w2, xf, gf, dw1, dw2t, ring, rbuf, acc, out_buf,
           load_sem, w_send, w_recv, x_send, x_recv, ring_sem, out_sem, row_send, row_recv, dep_send, dep_recv, own_sem, free_sem):
    d, c, r = lax.axis_index("dep"), lax.axis_index("col"), lax.axis_index("row")
    o = 1 - c
    across, layer, sibling = (d, o, r), (1 - d, c, r), (d, c, 1 - r)
    tokens, half = x_hbm.shape
    t = tokens // CHUNKS
    ffn = w1.shape[1]
    f = ffn // BLOCKS
    hf = BLOCKS // 2

    barrier = pltpu.get_barrier_semaphore()
    for peer in (across, layer, sibling):
        pl.semaphore_signal(barrier, inc=1, device_id=peer, device_id_type=MESH)
    pl.semaphore_wait(barrier, 3)

    def remote(src, dst, send, recv, dev):
        return pltpu.make_async_remote_copy(src_ref=src, dst_ref=dst, send_sem=send, recv_sem=recv, device_id=dev, device_id_type=MESH)

    def al(v, m):
        return pl.multiple_of(v, m)

    wts = ((w1_hbm, w1), (w2_hbm, w2))

    def w_copy(k, what):
        hbm, ref = wts[k]
        rows, cols = hbm.shape
        hr = rows // 2
        mine = lambda dep, col: ref.at[pl.ds(al(r * rows + dep * hr, hr), hr), pl.ds(al(col * cols, cols), cols)]
        if what == 0:
            return remote(hbm.at[pl.ds(al(d * hr, hr), hr), :], mine(d, c), w_send.at[k, 0], w_recv.at[k, 0], across)
        if what == 1:
            return remote(hbm, ref.at[pl.ds(al(r * rows, rows), rows), pl.ds(al(c * cols, cols), cols)], w_send.at[k, 1], w_recv.at[k, 1], sibling)
        if what == 2:
            return remote(mine(d, o), mine(d, o), w_send.at[k, 2], w_recv.at[k, 2], layer)
        if what == 3:
            return remote(mine(d, o), mine(d, o), w_send.at[k, 3], w_recv.at[k, 3], sibling)
        if what == 4:
            return remote(mine(1 - d, o), mine(1 - d, o), w_send.at[k, 4], w_recv.at[k, 4], sibling)
        return pltpu.make_async_copy(hbm, ref.at[pl.ds(al(r * rows, rows), rows), pl.ds(al(c * cols, cols), cols)], load_sem.at[k])

    acts = ((x_hbm, xf), (g_hbm, gf))

    def act_copy(k, i):
        hbm, ref = acts[k]
        rows = pl.ds(al(i * t, t), t)
        return remote(hbm.at[rows, :], ref.at[rows, pl.ds(al(c * half, half), half)], x_send.at[k, i], x_recv.at[k, i], across)

    def act_load(k):
        hbm, ref = acts[k]
        return pltpu.make_async_copy(hbm, ref.at[:, pl.ds(al(c * half, half), half)], load_sem.at[2 + k])

    for k in range(2):
        w_copy(k, 0).start()
        w_copy(k, 1).start()
        w_copy(k, 5).start()
    for k in range(2):
        act_load(k).start()
    for i in range(AHEAD):
        act_copy(0, i).start()

    dw1[...] = jnp.zeros_like(dw1)
    dw2t[...] = jnp.zeros_like(dw2t)
    for k in range(2):
        w_copy(k, 0).wait_recv()
        w_copy(k, 2).start()
        w_copy(k, 3).start()
    for k in range(2):
        w_copy(k, 5).wait()
        w_copy(k, 1).wait_recv()
        act_load(k).wait()
    w_copy(0, 2).wait_recv()
    w_copy(0, 4).start()
    w_copy(0, 3).wait_recv()
    w_copy(0, 4).wait_recv()

    def block_of(jj):
        return lax.rem(c * hf + jj, BLOCKS)

    def slope_copy(i, jj, slot, out):
        far = slope_hbm.at[i, jj]
        near = ring.at[slot]
        return pltpu.make_async_copy(near, far, ring_sem.at[slot]) if out else pltpu.make_async_copy(far, near, ring_sem.at[slot])

    def put(ref, i):
        return pltpu.make_async_copy(out_buf, ref.at[pl.ds(al(i * t, t), t), :], out_sem.at[0])

    own_cols = pl.ds(al(c * half, half), half)

    @pl.loop(0, CHUNKS)
    def _(i):
        rows = pl.ds(al(i * t, t), t)
        act_copy(0, i).wait_recv()

        @pl.when(i < CHUNKS - AHEAD)
        def _():
            act_copy(0, i + AHEAD).start()

        @pl.when(i >= CHUNKS - AHEAD)
        def _():
            act_copy(1, i + AHEAD - CHUNKS).start()

        @pl.loop(0, BLOCKS)
        def _(jj):
            n = i * BLOCKS + jj
            slot = lax.rem(n, RING)
            cols = pl.ds(al(block_of(jj) * f, f), f)
            u = dot(xf[rows, :], w1[:, cols])
            a, slope = gelu_and_slope(u)

            @pl.when(n >= RING)
            def _():
                slope_copy(i, jj, slot, True).wait()
            ring[slot] = slope
            slope_copy(i, jj, slot, True).start()
            a = a.astype(BF16)
            y = dot(a, w2[cols, own_cols])

            @pl.when(jj == 0)
            def _():
                acc[...] = y

            @pl.when(jj > 0)
            def _():
                acc[...] += y
            dw2t[:, cols] += dot(gf[rows, own_cols], a, 0, 0)

        @pl.when(i >= 1)
        def _():
            put(y_hbm, i).wait()
        out_buf[...] = acc[...].astype(BF16)
        put(y_hbm, i).start()

        @pl.when(i == 1)
        def _():
            w_copy(1, 2).wait_recv()
            w_copy(1, 4).start()
            w_copy(1, 3).wait_recv()

    for s in range(RING):
        slope_copy(0, 0, s, True).wait()
    for s in range(RING - 1):
        slope_copy(0, s, s, False).start()

    hcols = ffn // 2
    qcols = ffn // 4
    other_r = pl.ds(al((1 - r) * hcols, hcols), hcols)
    mine_r = pl.ds(al(r * hcols, hcols), hcols)

    def dw2_row():
        return remote(dw2t.at[:, other_r], rbuf, row_send.at[0], row_recv.at[0], sibling)

    def dw2_dep():
        return remote(dw2t.at[:, pl.ds(al(r * hcols + (1 - d) * qcols, qcols), qcols)], dw2_got, dep_send.at[0], dep_recv.at[0], layer)

    def dw2_out():
        return pltpu.make_async_copy(dw2t.at[:, pl.ds(al(r * hcols + d * qcols, qcols), qcols)], dw2_own, own_sem.at[0])

    dw2_row().start()
    w_copy(1, 4).wait_recv()
    put(y_hbm, 0).wait()
    dw2_row().wait_recv()
    dw2t[:, mine_r] += rbuf[...]
    pl.semaphore_signal(free_sem, inc=1, device_id=sibling, device_id_type=MESH)
    dw2_dep().start()
    dw2_out().start()

    @pl.loop(0, CHUNKS)
    def _(i):
        rows = pl.ds(al(i * t, t), t)
        act_copy(1, i).wait_recv()

        @pl.when(i < CHUNKS - AHEAD)
        def _():
            act_copy(1, i + AHEAD).start()

        def step(jj, with_dw1):
            n = i * BLOCKS + jj
            slot = lax.rem(n, RING)
            j = block_of(jj)
            cols = pl.ds(al(j * f, f), f)
            slope_copy(i, jj, slot, False).wait()

            @pl.when(n + RING - 1 < CHUNKS * BLOCKS)
            def _():
                m = n + RING - 1
                slope_copy(m // BLOCKS, lax.rem(m, BLOCKS), lax.rem(m, RING), False).start()
            da = dot(gf[rows, :], w2[cols, :], 1, 1)
            du = (da * ring[slot]).astype(BF16)
            dx = dot(du, w1[own_cols, cols], 1, 1)

            @pl.when(jj == 0)
            def _():
                acc[...] = dx

            @pl.when(jj > 0)
            def _():
                acc[...] += dx
            if with_dw1:
                dw1[:, pl.ds(al(jj * f, f), f)] += dot(xf[rows, :], du, 0, 0)

        @pl.loop(0, hf)
        def _(jj):
            step(jj, True)

        @pl.loop(hf, BLOCKS)
        def _(jj):
            step(jj, False)

        @pl.when(i >= 1)
        def _():
            put(dx_hbm, i).wait()
        out_buf[...] = acc[...].astype(BF16)
        put(dx_hbm, i).start()

    def dw1_row():
        return remote(dw1.at[pl.ds(al((1 - r) * half, half), half), :], rbuf, row_send.at[1], row_recv.at[1], sibling)

    q = half // 2

    def dw1_dep():
        return remote(dw1.at[pl.ds(al(r * half + (1 - d) * q, q), q), :], dw1_got, dep_send.at[1], dep_recv.at[1], layer)

    def dw1_out():
        return pltpu.make_async_copy(dw1.at[pl.ds(al(r * half + d * q, q), q), :], dw1_own, own_sem.at[1])

    pl.semaphore_wait(free_sem, 1)
    dw1_row().start()
    dw1_row().wait_recv()
    dw1[pl.ds(al(r * half, half), half), :] += rbuf[...]
    dw1_dep().start()
    dw1_out().start()

    for k in range(2):
        for what in range(5):
            w_copy(k, what).wait_send()
        for i in range(CHUNKS):
            act_copy(k, i).wait_send()
    put(dx_hbm, 0).wait()
    dw2_row().wait_send()
    dw2_dep().wait()
    dw2_out().wait()
    dw1_row().wait_send()
    dw1_dep().wait()
    dw1_out().wait()


def solution(mesh):
    act_spec = P(("dep", "row"), "col")
    wgt_spec = P("row", "col")
    grad_spec = P(("row", "dep"), "col")

    def local_block(x, w1, w2, g):
        tokens, half = x.shape
        hidden, hcols = w1.shape[0] * 2, w1.shape[1]
        ffn = hcols * 2
        t, f = tokens // CHUNKS, ffn // BLOCKS
        sds = jax.ShapeDtypeStruct
        dma = pltpu.SemaphoreType.DMA
        outs = pl.pallas_call(
            kernel,
            out_shape=[
                sds((tokens, half), BF16), sds((tokens, half), BF16),
                sds((half // 2, hcols), F32), sds((half // 2, hcols), F32),
                sds((half, ffn // 4), F32), sds((half, ffn // 4), F32),
                sds((CHUNKS, BLOCKS, t, f), F32),
            ],
            in_specs=[pl.BlockSpec(memory_space=pl.ANY)] * 4,
            out_specs=[pl.BlockSpec(memory_space=pl.ANY)] * 7,
            scratch_shapes=[
                pltpu.VMEM((hidden, ffn), BF16), pltpu.VMEM((ffn, hidden), BF16),
                pltpu.VMEM((tokens, hidden), BF16), pltpu.VMEM((tokens, hidden), BF16),
                pltpu.VMEM((hidden, hcols), F32), pltpu.VMEM((half, ffn), F32),
                pltpu.VMEM((RING, t, f), F32), pltpu.VMEM((half, hcols), F32),
                pltpu.VMEM((t, half), F32), pltpu.VMEM((t, half), BF16),
                dma((4,)), dma((2, 5)), dma((2, 5)), dma((2, CHUNKS)), dma((2, CHUNKS)),
                dma((RING,)), dma((2,)), dma((2,)), dma((2,)), dma((2,)), dma((2,)), dma((2,)),
                pltpu.SemaphoreType.REGULAR,
            ],
            compiler_params=pltpu.CompilerParams(collective_id=0, has_side_effects=True, vmem_limit_bytes=67043328),
            name="mlp_block",
        )(x, w1, w2, g)
        y, dx, dw1_own, dw1_got, dw2_own, dw2_got, _ = outs
        return y, dx, dw1_own + dw1_got, (dw2_own + dw2_got).T

    return jax.shard_map(local_block, mesh=mesh, in_specs=(act_spec, wgt_spec, wgt_spec, act_spec), out_specs=(act_spec, act_spec, grad_spec, grad_spec), check_vma=False)
```

```python
import functools

import jax
import jax.numpy as jnp
from jax import lax
from jax.experimental import pallas as pl
from jax.experimental.pallas import tpu as pltpu
from jax.sharding import PartitionSpec as P

GELU_COEF = 0.7978845608028654
CUBIC_COEF = 0.044715
MESH = pl.DeviceIdType.MESH
F32, BF16 = jnp.float32, jnp.bfloat16
CHUNKS = 8
BLOCKS = 8
RING = 4
AHEAD = 4


def gelu_and_slope(u):
    u2 = u * u
    p = GELU_COEF * CUBIC_COEF * u2 + GELU_COEF
    s = 0.5 * jnp.tanh(u * p) + 0.5
    a = u * s
    return a, s + (a * (1.0 - s)) * (6.0 * GELU_COEF * CUBIC_COEF * u2 + 2.0 * GELU_COEF)


def dot(a, b, ca=1, cb=0):
    return lax.dot_general(a, b, (((ca,), (cb,)), ((), ())), preferred_element_type=F32)


def kernel(x_hbm, w1_hbm, w2_hbm, g_hbm, y_hbm, dx_hbm, dw1_own, dw1_got, dw2_own, dw2_got, slope_hbm, part_hbm,
           w1, w2, xf, gf, dw1, dw2t, ring, acc, out_buf,
           load_sem, w_send, w_recv, x_send, x_recv, ring_sem, acc_sem, out_sem, row_send, row_recv, dep_send, dep_recv, own_sem, free_sem):
    d, c, r = lax.axis_index("dep"), lax.axis_index("col"), lax.axis_index("row")
    o = 1 - c
    across, layer, sibling = (d, o, r), (1 - d, c, r), (d, c, 1 - r)
    tokens, half = x_hbm.shape
    t = tokens // CHUNKS
    ffn = w1.shape[1]
    f = ffn // BLOCKS
    hf = BLOCKS // 2
    hcols, qcols, q = ffn // 2, ffn // 4, half // 2

    barrier = pltpu.get_barrier_semaphore()
    for peer in (across, layer, sibling):
        pl.semaphore_signal(barrier, inc=1, device_id=peer, device_id_type=MESH)
    pl.semaphore_wait(barrier, 3)

    def remote(src, dst, send, recv, dev):
        return pltpu.make_async_remote_copy(src_ref=src, dst_ref=dst, send_sem=send, recv_sem=recv, device_id=dev, device_id_type=MESH)

    def al(v, m):
        return pl.multiple_of(v, m)

    wts = ((w1_hbm, w1), (w2_hbm, w2))

    def w_copy(k, what):
        hbm, ref = wts[k]
        rows, cols = hbm.shape
        hr = rows // 2

        def part(dep, col):
            return ref.at[pl.ds(al(r * rows + dep * hr, hr), hr), pl.ds(al(col * cols, cols), cols)]

        def whole(col):
            return ref.at[pl.ds(al(r * rows, rows), rows), pl.ds(al(col * cols, cols), cols)]

        if what == 5:
            return pltpu.make_async_copy(hbm, whole(c), load_sem.at[k])
        src, dst, dev = (
            (hbm.at[pl.ds(al(d * hr, hr), hr), :], part(d, c), across),
            (hbm, whole(c), sibling),
            (part(d, o), part(d, o), layer),
            (part(d, o), part(d, o), sibling),
            (part(1 - d, o), part(1 - d, o), sibling),
            None,
            (hbm, whole(c), across),
            (whole(o), whole(o), sibling),
        )[what]
        return remote(src, dst, w_send.at[k, what], w_recv.at[k, what], dev)

    acts = ((x_hbm, xf), (g_hbm, gf))

    def act_copy(k, i):
        hbm, ref = acts[k]
        rows = pl.ds(al(i * t, t), t)
        return remote(hbm.at[rows, :], ref.at[rows, pl.ds(al(c * half, half), half)], x_send.at[k, i], x_recv.at[k, i], across)

    def act_load(k):
        hbm, ref = acts[k]
        return pltpu.make_async_copy(hbm, ref.at[:, pl.ds(al(c * half, half), half)], load_sem.at[2 + k])

    w_copy(0, 0).start()
    for i in range(AHEAD):
        act_copy(0, i).start()
    for k in range(2):
        w_copy(k, 5).start()
        w_copy(k, 1).start()
    for k in range(2):
        act_load(k).start()
    dw2t[...] = jnp.zeros_like(dw2t)
    w_copy(0, 0).wait_recv()
    w_copy(0, 2).start()
    w_copy(0, 3).start()
    for k in range(2):
        w_copy(k, 5).wait()
        w_copy(k, 1).wait_recv()
        act_load(k).wait()

    def block_of(jj):
        return lax.rem(c * hf + jj, BLOCKS)

    def slope_out(i, jj, slot):
        return pltpu.make_async_copy(ring.at[slot], slope_hbm.at[i, jj], ring_sem.at[slot])

    def slope_in(m):
        n = lax.rem(m, CHUNKS * hf)
        jj = (m // (CHUNKS * hf)) * hf + lax.rem(n, hf)
        slot = lax.rem(m, RING)
        return pltpu.make_async_copy(slope_hbm.at[n // hf, jj], ring.at[slot], ring_sem.at[slot])

    def put(ref, i):
        return pltpu.make_async_copy(out_buf, ref.at[pl.ds(al(i * t, t), t), :], out_sem.at[0])

    own_cols = pl.ds(al(c * half, half), half)

    @pl.loop(0, CHUNKS)
    def _(i):
        rows = pl.ds(al(i * t, t), t)
        act_copy(0, i).wait_recv()

        @pl.when(i < CHUNKS - AHEAD)
        def _():
            act_copy(0, i + AHEAD).start()

        @pl.when((i == CHUNKS - AHEAD) & (r != c))
        def _():
            w_copy(1, 0).start()

        @pl.when(i >= CHUNKS - AHEAD)
        def _():
            act_copy(1, i + AHEAD - CHUNKS).start()

        acc[0] = jnp.zeros_like(acc[0])

        @pl.loop(0, BLOCKS)
        def _(jj):
            n = i * BLOCKS + jj
            slot = lax.rem(n, RING)
            cols = pl.ds(al(block_of(jj) * f, f), f)

            @pl.when(n >= RING)
            def _():
                slope_out(i, jj, slot).wait()

            @pl.when(n == hf)
            def _():
                w_copy(0, 2).wait_recv()
                w_copy(0, 4).start()
                w_copy(0, 3).wait_recv()
                w_copy(0, 4).wait_recv()

            u = dot(xf[rows, :], w1[:, cols])
            a, slope = gelu_and_slope(u)
            ring[slot] = slope
            a = a.astype(BF16)
            acc[0] += dot(a, w2[cols, own_cols])
            dw2t[:, cols] += dot(gf[rows, own_cols], a, 0, 0)
            slope_out(i, jj, slot).start()

        @pl.when(i >= 1)
        def _():
            put(y_hbm, i).wait()
        out_buf[...] = acc[0].astype(BF16)
        put(y_hbm, i).start()

    other_r = pl.ds(al((1 - r) * hcols, hcols), hcols)
    mine_r = pl.ds(al(r * hcols, hcols), hcols)
    landing = dw1.at[0:half, :]

    def dw2_row():
        return remote(dw2t.at[:, other_r], landing, row_send.at[0], row_recv.at[0], sibling)

    def dw2_dep():
        return remote(dw2t.at[:, pl.ds(al(r * hcols + (1 - d) * qcols, qcols), qcols)], dw2_got, dep_send.at[0], dep_recv.at[0], layer)

    def dw2_out():
        return pltpu.make_async_copy(dw2t.at[:, pl.ds(al(r * hcols + d * qcols, qcols), qcols)], dw2_own, own_sem.at[0])

    dw2_row().start()
    for s in range(RING):
        slope_out(0, 0, s).wait()
    for m in range(RING - 1):
        slope_in(m).start()
    put(y_hbm, 0).wait()

    @pl.when(r == c)
    def _():
        w_copy(1, 0).wait_recv()
        w_copy(1, 2).start()
        w_copy(1, 3).start()

    dw2_row().wait_recv()
    dw2t[:, mine_r] += landing[...]
    dw2_dep().start()
    dw2_out().start()
    dw1[...] = jnp.zeros_like(dw1)

    @pl.when(r == c)
    def _():
        w_copy(1, 2).wait_recv()
        w_copy(1, 4).start()

    @pl.when(r != c)
    def _():
        w_copy(1, 3).wait_recv()
        w_copy(1, 4).wait_recv()

    def backward(i, jj, m, slot):
        rows = pl.ds(al(i * t, t), t)
        cols = pl.ds(al(block_of(jj) * f, f), f)
        slope_in(m).wait()

        @pl.when(m + RING - 1 < CHUNKS * BLOCKS)
        def _():
            slope_in(m + RING - 1).start()
        da = dot(gf[rows, :], w2[cols, :], 1, 1)
        du = (da * ring[lax.rem(m, RING)]).astype(BF16)
        acc[slot] += dot(du, w1[own_cols, cols], 1, 1)
        return rows, du

    def part_copy(i, out):
        far, near, sem = part_hbm.at[i], acc.at[lax.rem(i, 2)], acc_sem.at[lax.rem(i, 2)]
        return pltpu.make_async_copy(near, far, sem) if out else pltpu.make_async_copy(far, near, sem)

    @pl.loop(0, CHUNKS)
    def _(i):
        slot = lax.rem(i, 2)

        @pl.when(i >= 2)
        def _():
            part_copy(i, True).wait()
        act_copy(1, i).wait_recv()

        @pl.when(i < CHUNKS - AHEAD)
        def _():
            act_copy(1, i + AHEAD).start()

        @pl.when((i == CHUNKS - AHEAD) & (r == c))
        def _():
            w_copy(1, 6).start()

        @pl.when(i == CHUNKS - 2)
        def _():
            dw2_row().wait_send()
            dw2_dep().wait_send()
            dw2_out().wait()
            pl.semaphore_signal(free_sem, inc=1, device_id=sibling, device_id_type=MESH)

        acc[slot] = jnp.zeros_like(acc[slot])

        @pl.loop(0, hf)
        def _(jj):
            rows, du = backward(i, jj, i * hf + jj, slot)
            dw1[:, pl.ds(al(jj * f, f), f)] += dot(xf[rows, :], du, 0, 0)

        part_copy(i, True).start()

    def dw1_row(b):
        cols = pl.ds(b * f, f)
        return remote(dw1.at[pl.ds(al((1 - r) * half, half), half), cols], dw2t.at[:, cols], row_send.at[1 + b], row_recv.at[1 + b], sibling)

    def dw1_dep(b):
        cols = pl.ds(b * f, f)
        return remote(dw1.at[pl.ds(al(r * half + (1 - d) * q, q), q), cols], dw1_got.at[:, cols], dep_send.at[1 + b], dep_recv.at[1 + b], layer)

    def dw1_out():
        return pltpu.make_async_copy(dw1.at[pl.ds(al(r * half + d * q, q), q), :], dw1_own, own_sem.at[1])

    pl.semaphore_wait(free_sem, 1)
    for b in range(hf):
        dw1_row(b).start()
    for b in range(hf):
        dw1_row(b).wait_recv()
        dw1[pl.ds(al(r * half, half), half), b * f:(b + 1) * f] += dw2t[:, b * f:(b + 1) * f]
        dw1_dep(b).start()
    dw1_out().start()

    @pl.when(r != c)
    def _():
        w_copy(1, 6).wait_recv()
        w_copy(1, 7).start()

    @pl.when(r == c)
    def _():
        w_copy(1, 7).wait_recv()

    for i in (0, 1):
        part_copy(i, True).wait()
    part_copy(0, False).start()

    @pl.loop(0, CHUNKS)
    def _(i):
        slot = lax.rem(i, 2)
        part_copy(i, False).wait()

        @pl.when(i < CHUNKS - 1)
        def _():
            part_copy(i + 1, False).start()

        @pl.loop(0, hf)
        def _(jj):
            backward(i, hf + jj, CHUNKS * hf + i * hf + jj, slot)

        @pl.when(i >= 1)
        def _():
            put(dx_hbm, i).wait()
        out_buf[...] = acc[slot].astype(BF16)
        put(dx_hbm, i).start()

    for what in (0, 1, 2, 3, 4):
        w_copy(0, what).wait_send()
    w_copy(1, 1).wait_send()

    @pl.when(r != c)
    def _():
        w_copy(1, 0).wait_send()
        w_copy(1, 7).wait_send()

    @pl.when(r == c)
    def _():
        for what in (2, 3, 4, 6):
            w_copy(1, what).wait_send()

    for k in range(2):
        for i in range(CHUNKS):
            act_copy(k, i).wait_send()
    put(dx_hbm, 0).wait()
    dw2_dep().wait_recv()
    for b in range(hf):
        dw1_row(b).wait_send()
        dw1_dep(b).wait()
    dw1_out().wait()


def solution(mesh):
    act_spec = P(("dep", "row"), "col")
    wgt_spec = P("row", "col")
    grad_spec = P(("row", "dep"), "col")

    def local_block(x, w1, w2, g):
        tokens, half = x.shape
        hidden, hcols = w1.shape[0] * 2, w1.shape[1]
        ffn = hcols * 2
        t, f = tokens // CHUNKS, ffn // BLOCKS
        sds = jax.ShapeDtypeStruct
        dma = pltpu.SemaphoreType.DMA
        outs = pl.pallas_call(
            kernel,
            out_shape=[
                sds((tokens, half), BF16), sds((tokens, half), BF16),
                sds((half // 2, hcols), F32), sds((half // 2, hcols), F32),
                sds((half, ffn // 4), F32), sds((half, ffn // 4), F32),
                sds((CHUNKS, BLOCKS, t, f), F32), sds((CHUNKS, t, half), F32),
            ],
            in_specs=[pl.BlockSpec(memory_space=pl.ANY)] * 4,
            out_specs=[pl.BlockSpec(memory_space=pl.ANY)] * 8,
            scratch_shapes=[
                pltpu.VMEM((hidden, ffn), BF16), pltpu.VMEM((ffn, hidden), BF16),
                pltpu.VMEM((tokens, hidden), BF16), pltpu.VMEM((tokens, hidden), BF16),
                pltpu.VMEM((hidden, hcols), F32), pltpu.VMEM((half, ffn), F32),
                pltpu.VMEM((RING, t, f), F32), pltpu.VMEM((2, t, half), F32), pltpu.VMEM((t, half), BF16),
                dma((4,)), dma((2, 8)), dma((2, 8)), dma((2, CHUNKS)), dma((2, CHUNKS)),
                dma((RING,)), dma((2,)), dma((1,)),
                dma((1 + BLOCKS // 2,)), dma((1 + BLOCKS // 2,)), dma((1 + BLOCKS // 2,)), dma((1 + BLOCKS // 2,)), dma((2,)),
                pltpu.SemaphoreType.REGULAR,
            ],
            compiler_params=pltpu.CompilerParams(collective_id=0, has_side_effects=True, vmem_limit_bytes=67043328),
            name="mlp_block",
        )(x, w1, w2, g)
        y, dx, dw1_own, dw1_got, dw2_own, dw2_got, _, _ = outs
        return y, dx, dw1_own + dw1_got, (dw2_own + dw2_got).T

    return jax.shard_map(local_block, mesh=mesh, in_specs=(act_spec, wgt_spec, wgt_spec, act_spec), out_specs=(act_spec, act_spec, grad_spec, grad_spec), check_vma=False)
```

```python
import functools

import jax
import jax.numpy as jnp
from jax import lax
from jax.experimental import pallas as pl
from jax.experimental.pallas import tpu as pltpu
from jax.sharding import PartitionSpec as P

GELU_COEF = 0.7978845608028654
CUBIC_COEF = 0.044715
MESH = pl.DeviceIdType.MESH
F32, BF16 = jnp.float32, jnp.bfloat16
CHUNKS = 8
BLOCKS = 8
RING = 4
AHEAD = 4
SLOTS = 4
PIECES = 4


def gelu_and_slope(u):
    u2 = u * u
    p = GELU_COEF * CUBIC_COEF * u2 + GELU_COEF
    s = 0.5 * jnp.tanh(u * p) + 0.5
    a = u * s
    return a, s + (a * (1.0 - s)) * (6.0 * GELU_COEF * CUBIC_COEF * u2 + 2.0 * GELU_COEF)


def dot(a, b, ca=1, cb=0):
    return lax.dot_general(a, b, (((ca,), (cb,)), ((), ())), preferred_element_type=F32)


def kernel(x_hbm, w1_hbm, w2_hbm, g_hbm, y_hbm, dx_hbm, dw1_own, dw2_own, slope_hbm, part_hbm,
           w1, w2, xf, gf, dw1, dw2t, ring, acc, out_buf,
           load_sem, w_send, w_recv, x_send, x_recv, ring_sem, acc_sem, out_sem, row_send, row_recv, dep_send, dep_recv, own_sem, free_sem, room_sem):
    d, c, r = lax.axis_index("dep"), lax.axis_index("col"), lax.axis_index("row")
    o = 1 - c
    across, layer, sibling = (d, o, r), (1 - d, c, r), (d, c, 1 - r)
    tokens, half = x_hbm.shape
    t = tokens // CHUNKS
    ffn = w1.shape[1]
    f = ffn // BLOCKS
    hf = BLOCKS // 2
    hcols, qcols, q = ffn // 2, ffn // 4, half // 2

    barrier = pltpu.get_barrier_semaphore()
    for peer in (across, layer, sibling):
        pl.semaphore_signal(barrier, inc=1, device_id=peer, device_id_type=MESH)
    pl.semaphore_wait(barrier, 3)

    def remote(src, dst, send, recv, dev):
        return pltpu.make_async_remote_copy(src_ref=src, dst_ref=dst, send_sem=send, recv_sem=recv, device_id=dev, device_id_type=MESH)

    def al(v, m):
        return pl.multiple_of(v, m)

    wts = ((w1_hbm, w1), (w2_hbm, w2))

    def w_copy(k, what):
        hbm, ref = wts[k]
        rows, cols = hbm.shape

        def span(start, size, col):
            return ref.at[pl.ds(al(start, size), size), pl.ds(al(col * cols, cols), cols)]

        def part(dep, col):
            if k == 0:
                return span(r * rows + dep * (rows // 2), rows // 2, col)
            return span((1 - col) * rows + dep * (rows // 2) + r * (rows // 4), rows // 4, col)

        def late(col):
            return span(col * rows + (what // 8) * (rows // 2) + r * (rows // 4), rows // 4, col)

        block = span(r * rows, rows, c)
        if what == 5:
            return pltpu.make_async_copy(hbm, block, load_sem.at[k])
        if what >= 6:
            src, dst, dev = (late(c), late(c), across) if what % 2 == 0 else (late(o), late(o), sibling)
        else:
            src, dst, dev = (
                (hbm.at[pl.ds(al(d * (rows // 2), rows // 2), rows // 2), :] if k == 0 else part(d, c), part(d, c), across),
                (hbm, block, sibling),
                (part(d, o), part(d, o), layer),
                (part(d, o), part(d, o), sibling),
                (part(1 - d, o), part(1 - d, o), sibling),
            )[what]
        return remote(src, dst, w_send.at[k, what], w_recv.at[k, what], dev)

    acts = ((x_hbm, xf), (g_hbm, gf))

    def act_copy(k, i):
        hbm, ref = acts[k]
        rows = pl.ds(al(i * t, t), t)
        return remote(hbm.at[rows, :], ref.at[rows, pl.ds(al(c * half, half), half)], x_send.at[k, i], x_recv.at[k, i], across)

    def act_load(k):
        hbm, ref = acts[k]
        return pltpu.make_async_copy(hbm, ref.at[:, pl.ds(al(c * half, half), half)], load_sem.at[2 + k])

    w_copy(0, 0).start()
    for i in range(AHEAD):
        act_copy(0, i).start()
    for k in range(2):
        w_copy(k, 5).start()
        w_copy(k, 1).start()
    for k in range(2):
        act_load(k).start()
    dw2t[...] = jnp.zeros_like(dw2t)
    w_copy(0, 0).wait_recv()
    w_copy(0, 2).start()
    w_copy(0, 3).start()
    for k in range(2):
        w_copy(k, 5).wait()
        w_copy(k, 1).wait_recv()
        act_load(k).wait()

    def block_of(jj):
        return lax.rem(c * hf + jj, BLOCKS)

    def slope_out(i, jj, slot):
        return pltpu.make_async_copy(ring.at[slot], slope_hbm.at[i, jj], ring_sem.at[slot])

    def slope_in(m):
        first = CHUNKS * hf
        n = jnp.maximum(m - first, 0)
        i = jnp.where(m < first, m // hf, lax.rem(n, first // 2) // 2)
        jj = jnp.where(m < first, lax.rem(m, hf), hf + (n // (first // 2)) * 2 + lax.rem(n, 2))
        slot = lax.rem(m, RING)
        return pltpu.make_async_copy(slope_hbm.at[i, jj], ring.at[slot], ring_sem.at[slot])

    def put(ref, i):
        return pltpu.make_async_copy(out_buf, ref.at[pl.ds(al(i * t, t), t), :], out_sem.at[0])

    own_cols = pl.ds(al(c * half, half), half)

    @pl.loop(0, CHUNKS)
    def _(i):
        rows = pl.ds(al(i * t, t), t)
        act_copy(0, i).wait_recv()

        @pl.when(i < CHUNKS - AHEAD)
        def _():
            act_copy(0, i + AHEAD).start()

        @pl.when(i == CHUNKS - AHEAD)
        def _():
            w_copy(1, 0).start()

        @pl.when(i >= CHUNKS - AHEAD)
        def _():
            act_copy(1, i + AHEAD - CHUNKS).start()

        acc[0] = jnp.zeros_like(acc[0])

        @pl.loop(0, BLOCKS)
        def _(jj):
            n = i * BLOCKS + jj
            slot = lax.rem(n, RING)
            cols = pl.ds(al(block_of(jj) * f, f), f)

            @pl.when(n >= RING)
            def _():
                slope_out(i, jj, slot).wait()

            @pl.when(n == hf)
            def _():
                w_copy(0, 2).wait_recv()
                w_copy(0, 4).start()
                w_copy(0, 3).wait_recv()
                w_copy(0, 4).wait_recv()

            u = dot(xf[rows, :], w1[:, cols])
            a, slope = gelu_and_slope(u)
            ring[slot] = slope
            a = a.astype(BF16)
            acc[0] += dot(a, w2[cols, own_cols])
            dw2t[:, cols] += dot(gf[rows, own_cols], a, 0, 0)
            slope_out(i, jj, slot).start()

        @pl.when(i >= 1)
        def _():
            put(y_hbm, i).wait()
        out_buf[...] = acc[0].astype(BF16)
        put(y_hbm, i).start()

    other_r = pl.ds(al((1 - r) * hcols, hcols), hcols)
    mine_r = pl.ds(al(r * hcols, hcols), hcols)
    landing = dw1.at[0:half, :]

    def dw2_row():
        return remote(dw2t.at[:, other_r], landing, row_send.at[0], row_recv.at[0], sibling)

    dw2_landing = pl.ds(al((1 - r) * hcols, hcols), qcols)
    dw2_mine = pl.ds(al(r * hcols + d * qcols, qcols), qcols)

    def dw2_dep():
        return remote(dw2t.at[:, pl.ds(al(r * hcols + (1 - d) * qcols, qcols), qcols)], dw2t.at[:, dw2_landing], dep_send.at[0], dep_recv.at[0], layer)

    def dw2_out():
        return pltpu.make_async_copy(dw2t.at[:, dw2_mine], dw2_own, own_sem.at[0])

    dw2_row().start()
    for s in range(RING):
        slope_out(0, 0, s).wait()
    for m in range(RING - 1):
        slope_in(m).start()
    put(y_hbm, 0).wait()

    w_copy(1, 0).wait_recv()
    w_copy(1, 2).start()
    w_copy(1, 3).start()
    dw2_row().wait()
    pl.semaphore_signal(room_sem, inc=1, device_id=layer, device_id_type=MESH)
    dw2t[:, mine_r] += landing[...]
    pl.semaphore_wait(room_sem, 1)
    dw2_dep().start()
    dw1[...] = jnp.zeros_like(dw1)

    w_copy(1, 2).wait_recv()
    w_copy(1, 4).start()
    w_copy(1, 3).wait_recv()
    w_copy(1, 4).wait_recv()

    def backward(i, jj, m, slot):
        rows = pl.ds(al(i * t, t), t)
        cols = pl.ds(al(block_of(jj) * f, f), f)
        slope_in(m).wait()

        @pl.when(m + RING - 1 < CHUNKS * BLOCKS)
        def _():
            slope_in(m + RING - 1).start()
        da = dot(gf[rows, :], w2[cols, :], 1, 1)
        du = (da * ring[lax.rem(m, RING)]).astype(BF16)
        acc[slot] += dot(du, w1[own_cols, cols], 1, 1)
        return rows, du

    def part_copy(i, out):
        far, near, sem = part_hbm.at[lax.rem(i, CHUNKS)], acc.at[lax.rem(i, SLOTS)], acc_sem.at[lax.rem(i, SLOTS)]
        return pltpu.make_async_copy(near, far, sem) if out else pltpu.make_async_copy(far, near, sem)

    def dw1_row(b):
        cols = pl.ds(al(b * f, f), f)
        return remote(dw1.at[pl.ds(al((1 - r) * half, half), half), cols], dw2t.at[:, cols], row_send.at[1 + b], row_recv.at[1 + b], sibling)

    def dw1_dep(b):
        cols = pl.ds(al(b * f, f), f)
        return remote(dw1.at[pl.ds(al(r * half + (1 - d) * q, q), q), cols], dw2t.at[0:q, pl.ds(al(hcols + b * f, f), f)], dep_send.at[1 + b], dep_recv.at[1 + b], layer)

    def dw1_out(b):
        cols = pl.ds(al(b * f, f), f)
        return pltpu.make_async_copy(dw1.at[pl.ds(al(r * half + d * q, q), q), cols], dw1_own.at[:, cols], own_sem.at[1 + b])

    def dw1_pass_on(b):
        cols = pl.ds(al(b * f, f), f)
        dw1_row(b).wait_recv()
        dw1[pl.ds(al(r * half, half), half), cols] += dw2t[:, cols]
        dw1_dep(b).start()

    @pl.loop(0, CHUNKS)
    def _(i):
        slot = lax.rem(i, SLOTS)

        @pl.when(i >= SLOTS)
        def _():
            part_copy(i, True).wait()
        act_copy(1, i).wait_recv()

        @pl.when(i < CHUNKS - AHEAD)
        def _():
            act_copy(1, i + AHEAD).start()

        @pl.when(i == CHUNKS - AHEAD)
        def _():
            w_copy(1, 6).start()
            w_copy(1, 8).start()

        @pl.when(i == CHUNKS - 2)
        def _():
            dw2_dep().wait()
            dw2t[:, dw2_mine] += dw2t[:, dw2_landing]
            dw2_out().start()

        @pl.when(i == CHUNKS - 1)
        def _():
            dw2_out().wait()
            for peer in (sibling, layer):
                pl.semaphore_signal(free_sem, inc=1, device_id=peer, device_id_type=MESH)

        acc[slot] = jnp.zeros_like(acc[slot])

        @pl.loop(0, hf)
        def _(jj):
            rows, du = backward(i, jj, i * hf + jj, slot)
            dw1[:, pl.ds(al(jj * f, f), f)] += dot(xf[rows, :], du, 0, 0)

            @pl.when(i == CHUNKS - 1)
            def _():
                @pl.when(jj == 0)
                def _():
                    pl.semaphore_wait(free_sem, 2)
                dw1_row(jj).start()

                @pl.when(jj >= 2)
                def _():
                    dw1_pass_on(jj - 2)

        part_copy(i, True).start()

    for b in range(hf - 2, hf):
        dw1_pass_on(b)
    for i in (0, 1):
        part_copy(i, True).wait()
        part_copy(i, False).start()
    w_copy(1, 6).wait_recv()
    w_copy(1, 7).start()
    w_copy(1, 7).wait_recv()

    @pl.loop(0, 2 * CHUNKS)
    def _(k):
        last = k // CHUNKS
        i = lax.rem(k, CHUNKS)
        slot = lax.rem(k, SLOTS)
        part_copy(k, False).wait()

        @pl.when(k < CHUNKS + 2)
        def _():
            part_copy(k + 2, True).wait()

        @pl.when(k < 2 * CHUNKS - 2)
        def _():
            part_copy(k + 2, False).start()

        @pl.when(k == CHUNKS)
        def _():
            w_copy(1, 8).wait_recv()
            w_copy(1, 9).start()
            w_copy(1, 9).wait_recv()

        @pl.loop(0, 2)
        def _(b):
            backward(i, hf + 2 * last + b, CHUNKS * hf + 2 * k + b, slot)

        @pl.when(last == 0)
        def _():
            part_copy(k, True).start()

        @pl.when(last == 1)
        def _():
            @pl.when(i >= 1)
            def _():
                put(dx_hbm, i).wait()
            out_buf[...] = acc[slot].astype(BF16)
            put(dx_hbm, i).start()

    for what in (0, 1, 2, 3, 4):
        for k in range(2):
            w_copy(k, what).wait_send()
    for what in (6, 7, 8, 9):
        w_copy(1, what).wait_send()
    for k in range(2):
        for i in range(CHUNKS):
            act_copy(k, i).wait_send()
    put(dx_hbm, 0).wait()
    for b in range(hf):
        dw1_dep(b).wait_recv()
        dw1[pl.ds(al(r * half + d * q, q), q), b * f:(b + 1) * f] += dw2t[0:q, hcols + b * f:hcols + (b + 1) * f]
        dw1_out(b).start()
    for b in range(hf):
        dw1_row(b).wait_send()
        dw1_dep(b).wait_send()
        dw1_out(b).wait()


def finish_kernel(y_in, dx_in, dw1_in, dw2_in, y_out, dx_out, dw1_out, dw2_out, y, dx, dw1, dw2t, dw2, in_sem, out_sem):
    copies = []
    for src, buf, dst, n in ((dw2_in, dw2t, None, PIECES), (y_in, y, y_out, PIECES), (dx_in, dx, dx_out, PIECES), (dw1_in, dw1, dw1_out, PIECES // 2)):
        rows = src.shape[0] // n
        for p in range(n):
            sl = pl.ds(p * rows, rows)
            copies.append((src.at[sl, :], buf.at[sl, :], None if dst is None else dst.at[sl, :]))
    ins = [pltpu.make_async_copy(a, b, in_sem.at[k]) for k, (a, b, _) in enumerate(copies)]
    for cp in ins:
        cp.start()
    outs = []
    for k, (_, b, o) in enumerate(copies):
        ins[k].wait()
        if o is None:
            rows = dw2t.shape[0] // PIECES
            dw2[:, k * rows:(k + 1) * rows] = dw2t[k * rows:(k + 1) * rows, :].T
            if k == PIECES - 1:
                outs.append(pltpu.make_async_copy(dw2, dw2_out, out_sem.at[k]))
                outs[-1].start()
        else:
            outs.append(pltpu.make_async_copy(b, o, out_sem.at[k]))
            outs[-1].start()
    for cp in outs:
        cp.wait()


def finish(y, dx, dw1, dw2t):
    sds = jax.ShapeDtypeStruct
    n = 3 * PIECES + PIECES // 2
    return pl.pallas_call(
        finish_kernel,
        out_shape=[sds(y.shape, BF16), sds(dx.shape, BF16), sds(dw1.shape, F32), sds(dw2t.shape[::-1], F32)],
        in_specs=[pl.BlockSpec(memory_space=pl.ANY)] * 4,
        out_specs=[pl.BlockSpec(memory_space=pl.ANY)] * 4,
        scratch_shapes=[
            pltpu.VMEM(y.shape, BF16), pltpu.VMEM(dx.shape, BF16), pltpu.VMEM(dw1.shape, F32),
            pltpu.VMEM(dw2t.shape, F32), pltpu.VMEM(dw2t.shape[::-1], F32),
            pltpu.SemaphoreType.DMA((n,)), pltpu.SemaphoreType.DMA((n,)),
        ],
        compiler_params=pltpu.CompilerParams(vmem_limit_bytes=60 * 1024 * 1024),
        name="finish",
    )(y, dx, dw1, dw2t)


def solution(mesh):
    act_spec = P(("dep", "row"), "col")
    wgt_spec = P("row", "col")
    grad_spec = P(("row", "dep"), "col")

    def local_block(x, w1, w2, g):
        tokens, half = x.shape
        hidden, hcols = w1.shape[0] * 2, w1.shape[1]
        ffn = hcols * 2
        t, f = tokens // CHUNKS, ffn // BLOCKS
        sds = jax.ShapeDtypeStruct
        dma = pltpu.SemaphoreType.DMA
        outs = pl.pallas_call(
            kernel,
            out_shape=[
                sds((tokens, half), BF16), sds((tokens, half), BF16),
                sds((half // 2, hcols), F32),
                sds((half, ffn // 4), F32),
                sds((CHUNKS, BLOCKS, t, f), F32), sds((CHUNKS, t, half), F32),
            ],
            in_specs=[pl.BlockSpec(memory_space=pl.ANY)] * 4,
            out_specs=[pl.BlockSpec(memory_space=pl.ANY)] * 6,
            scratch_shapes=[
                pltpu.VMEM((hidden, ffn), BF16), pltpu.VMEM((ffn, hidden), BF16),
                pltpu.VMEM((tokens, hidden), BF16), pltpu.VMEM((tokens, hidden), BF16),
                pltpu.VMEM((hidden, hcols), F32), pltpu.VMEM((half, ffn), F32),
                pltpu.VMEM((RING, t, f), F32), pltpu.VMEM((SLOTS, t, half), F32), pltpu.VMEM((t, half), BF16),
                dma((4,)), dma((2, 10)), dma((2, 10)), dma((2, CHUNKS)), dma((2, CHUNKS)),
                dma((RING,)), dma((SLOTS,)), dma((1,)),
                dma((1 + BLOCKS // 2,)), dma((1 + BLOCKS // 2,)), dma((1 + BLOCKS // 2,)), dma((1 + BLOCKS // 2,)), dma((1 + BLOCKS // 2,)),
                pltpu.SemaphoreType.REGULAR, pltpu.SemaphoreType.REGULAR,
            ],
            compiler_params=pltpu.CompilerParams(collective_id=0, has_side_effects=True, vmem_limit_bytes=67043328),
            name="mlp_block",
        )(x, w1, w2, g)
        return finish(*outs[:4])

    return jax.shard_map(local_block, mesh=mesh, in_specs=(act_spec, wgt_spec, wgt_spec, act_spec), out_specs=(act_spec, act_spec, grad_spec, grad_spec), check_vma=False)
```

```python
import functools

import jax
import jax.numpy as jnp
from jax import lax
from jax.experimental import pallas as pl
from jax.experimental.pallas import tpu as pltpu
from jax.sharding import PartitionSpec as P

GELU_COEF = 0.7978845608028654
CUBIC_COEF = 0.044715
MESH = pl.DeviceIdType.MESH
F32, BF16 = jnp.float32, jnp.bfloat16
CHUNKS = 8
BLOCKS = 8
RING = 4
AHEAD = 4
SLOTS = 4
PIECES = 4


def gelu_and_slope(u):
    u2 = u * u
    p = GELU_COEF * CUBIC_COEF * u2 + GELU_COEF
    s = 0.5 * jnp.tanh(u * p) + 0.5
    a = u * s
    return a, s + (a * (1.0 - s)) * (6.0 * GELU_COEF * CUBIC_COEF * u2 + 2.0 * GELU_COEF)


def dot(a, b, ca=1, cb=0):
    return lax.dot_general(a, b, (((ca,), (cb,)), ((), ())), preferred_element_type=F32)


def kernel(x_hbm, w1_hbm, w2_hbm, g_hbm, y_hbm, dx_hbm, dw1_own, dw2_own, give_hbm, slope_hbm, part_hbm,
           w1, w2, xf, gf, dw1, dw2t, ring, acc, out_buf,
           load_sem, w_send, w_recv, x_send, x_recv, ring_sem, acc_sem, out_sem, row_send, row_recv, dep_send, dep_recv, own_sem, give_sem, free_sem, room_sem):
    d, c, r = lax.axis_index("dep"), lax.axis_index("col"), lax.axis_index("row")
    o = 1 - c
    across, layer, sibling = (d, o, r), (1 - d, c, r), (d, c, 1 - r)
    tokens, half = x_hbm.shape
    t = tokens // CHUNKS
    ffn = w1.shape[1]
    f = ffn // BLOCKS
    hf = BLOCKS // 2
    hcols, qcols, q = ffn // 2, ffn // 4, half // 2
    e = f // 2

    barrier = pltpu.get_barrier_semaphore()
    for peer in (across, layer, sibling):
        pl.semaphore_signal(barrier, inc=1, device_id=peer, device_id_type=MESH)
    pl.semaphore_wait(barrier, 3)

    def remote(src, dst, send, recv, dev):
        return pltpu.make_async_remote_copy(src_ref=src, dst_ref=dst, send_sem=send, recv_sem=recv, device_id=dev, device_id_type=MESH)

    def al(v, m):
        return pl.multiple_of(v, m)

    wts = ((w1_hbm, w1), (w2_hbm, w2))

    def w_copy(k, what):
        hbm, ref = wts[k]
        rows, cols = hbm.shape

        def span(start, size, col):
            return ref.at[pl.ds(al(start, size), size), pl.ds(al(col * cols, cols), cols)]

        def part(dep, col):
            if k == 0:
                return span(r * rows + dep * (rows // 2), rows // 2, col)
            return span((1 - col) * rows + dep * (rows // 2) + r * (rows // 4), rows // 4, col)

        def late(col):
            return span(col * rows + (what // 8) * (rows // 2) + r * (rows // 4), rows // 4, col)

        block = span(r * rows, rows, c)
        if what == 5:
            return pltpu.make_async_copy(hbm, block, load_sem.at[k])
        if what >= 6:
            src, dst, dev = (late(c), late(c), across) if what % 2 == 0 else (late(o), late(o), sibling)
        else:
            src, dst, dev = (
                (hbm.at[pl.ds(al(d * (rows // 2), rows // 2), rows // 2), :] if k == 0 else part(d, c), part(d, c), across),
                (hbm, block, sibling),
                (part(d, o), part(d, o), layer),
                (part(d, o), part(d, o), sibling),
                (part(1 - d, o), part(1 - d, o), sibling),
            )[what]
        return remote(src, dst, w_send.at[k, what], w_recv.at[k, what], dev)

    acts = ((x_hbm, xf), (g_hbm, gf))

    def act_copy(k, i):
        hbm, ref = acts[k]
        rows = pl.ds(al(i * t, t), t)
        return remote(hbm.at[rows, :], ref.at[rows, pl.ds(al(c * half, half), half)], x_send.at[k, i], x_recv.at[k, i], across)

    def act_load(k):
        hbm, ref = acts[k]
        return pltpu.make_async_copy(hbm, ref.at[:, pl.ds(al(c * half, half), half)], load_sem.at[2 + k])

    w_copy(0, 0).start()
    act_copy(0, 0).start()
    for k in range(2):
        w_copy(k, 5).start()
        w_copy(k, 1).start()
    for k in range(2):
        act_load(k).start()
    dw2t[...] = jnp.zeros_like(dw2t)
    w_copy(0, 0).wait_recv()
    w_copy(0, 2).start()
    w_copy(0, 3).start()
    for i in range(1, AHEAD):
        act_copy(0, i).start()
    for k in range(2):
        w_copy(k, 5).wait()
        w_copy(k, 1).wait_recv()
        act_load(k).wait()

    def block_of(jj):
        return lax.rem(c * hf + jj, BLOCKS)

    def slope_out(i, jj, slot):
        return pltpu.make_async_copy(ring.at[slot], slope_hbm.at[i, jj], ring_sem.at[slot])

    def slope_in(m):
        first = CHUNKS * hf
        n = jnp.maximum(m - first, 0)
        i = jnp.where(m < first, m // hf, lax.rem(n, first // 2) // 2)
        jj = jnp.where(m < first, lax.rem(m, hf), hf + (n // (first // 2)) * 2 + lax.rem(n, 2))
        slot = lax.rem(m, RING)
        return pltpu.make_async_copy(slope_hbm.at[i, jj], ring.at[slot], ring_sem.at[slot])

    def put(ref, i):
        return pltpu.make_async_copy(out_buf, ref.at[pl.ds(al(i * t, t), t), :], out_sem.at[0])

    own_cols = pl.ds(al(c * half, half), half)

    @pl.loop(0, CHUNKS)
    def _(i):
        rows = pl.ds(al(i * t, t), t)
        act_copy(0, i).wait_recv()

        @pl.when(i < CHUNKS - AHEAD)
        def _():
            act_copy(0, i + AHEAD).start()

        @pl.when(i == CHUNKS - AHEAD)
        def _():
            w_copy(1, 0).start()

        @pl.when(i >= CHUNKS - AHEAD)
        def _():
            act_copy(1, i + AHEAD - CHUNKS).start()

        acc[0] = jnp.zeros_like(acc[0])

        @pl.loop(0, BLOCKS)
        def _(jj):
            n = i * BLOCKS + jj
            slot = lax.rem(n, RING)
            cols = pl.ds(al(block_of(jj) * f, f), f)

            @pl.when(n >= RING)
            def _():
                slope_out(i, jj, slot).wait()

            @pl.when(n == hf)
            def _():
                w_copy(0, 2).wait_recv()
                w_copy(0, 4).start()
                w_copy(0, 3).wait_recv()
                w_copy(0, 4).wait_recv()

            u = dot(xf[rows, :], w1[:, cols])
            a, slope = gelu_and_slope(u)
            ring[slot] = slope
            a = a.astype(BF16)
            acc[0] += dot(a, w2[cols, own_cols])
            dw2t[:, cols] += dot(gf[rows, own_cols], a, 0, 0)
            slope_out(i, jj, slot).start()

        @pl.when(i >= 1)
        def _():
            put(y_hbm, i).wait()
        out_buf[...] = acc[0].astype(BF16)
        put(y_hbm, i).start()

    other_r = pl.ds(al((1 - r) * hcols, hcols), hcols)
    mine_r = pl.ds(al(r * hcols, hcols), hcols)
    landing = dw1.at[0:half, :]

    def dw2_row():
        return remote(dw2t.at[:, other_r], landing, row_send.at[0], row_recv.at[0], sibling)

    dw2_landing = pl.ds(al((1 - r) * hcols, hcols), qcols)
    dw2_mine = pl.ds(al(r * hcols + d * qcols, qcols), qcols)

    def dw2_dep():
        return remote(dw2t.at[:, pl.ds(al(r * hcols + (1 - d) * qcols, qcols), qcols)], dw2t.at[:, dw2_landing], dep_send.at[0], dep_recv.at[0], layer)

    def dw2_out():
        return pltpu.make_async_copy(dw2t.at[:, dw2_mine], dw2_own, own_sem.at[0])

    dw2_row().start()
    for s in range(RING):
        slope_out(0, 0, s).wait()
    for m in range(RING - 1):
        slope_in(m).start()
    put(y_hbm, 0).wait()

    w_copy(1, 0).wait_recv()
    w_copy(1, 2).start()
    w_copy(1, 3).start()
    dw2_row().wait()
    pl.semaphore_signal(room_sem, inc=1, device_id=layer, device_id_type=MESH)
    dw2t[:, mine_r] += landing[...]
    pl.semaphore_wait(room_sem, 1)
    dw2_dep().start()
    dw1[...] = jnp.zeros_like(dw1)

    w_copy(1, 2).wait_recv()
    w_copy(1, 4).start()
    w_copy(1, 3).wait_recv()
    w_copy(1, 4).wait_recv()

    def backward(i, jj, m, slot):
        rows = pl.ds(al(i * t, t), t)
        cols = pl.ds(al(block_of(jj) * f, f), f)
        slope_in(m).wait()
        slope_in(m + RING - 1).start()
        da = dot(gf[rows, :], w2[cols, :], 1, 1)
        du = (da * ring[lax.rem(m, RING)]).astype(BF16)
        acc[slot] += dot(du, w1[own_cols, cols], 1, 1)
        return rows, du

    def part_copy(i, out):
        far, near, sem = part_hbm.at[lax.rem(i, CHUNKS)], acc.at[lax.rem(i, SLOTS)], acc_sem.at[lax.rem(i, SLOTS)]
        return pltpu.make_async_copy(near, far, sem) if out else pltpu.make_async_copy(far, near, sem)

    def dw1_row(b):
        cols = pl.ds(al(b * f, f), f)
        return remote(dw1.at[pl.ds(al((1 - r) * half, half), half), cols], dw2t.at[:, cols], row_send.at[1 + b], row_recv.at[1 + b], sibling)

    def dw1_dep(b, width=f):
        src = dw1.at[pl.ds(al(r * half + (1 - d) * q, q), q), pl.ds(al(b * f, f), width)]
        dst = dw2t.at[0:q, pl.ds(al(hcols + b * f, f), width)]
        return remote(src, dst, dep_send.at[1 + b], dep_recv.at[1 + b], layer)

    def dw1_out(b):
        cols = pl.ds(al(b * f, f), f)
        return pltpu.make_async_copy(dw1.at[pl.ds(al(r * half + d * q, q), q), cols], dw1_own.at[:, cols], own_sem.at[1 + b])

    def dw1_take(b):
        cols = pl.ds(al(b * f, f), f)
        dw1_row(b).wait_recv()
        dw1[pl.ds(al(r * half, half), half), cols] += dw2t[:, cols]

    def dw1_give():
        return pltpu.make_async_copy(dw1.at[pl.ds(al(r * half + (1 - d) * q, q), q), pl.ds(hcols - e, e)], give_hbm, give_sem.at[0])

    @pl.loop(0, CHUNKS)
    def _(i):
        slot = lax.rem(i, SLOTS)

        @pl.when(i >= SLOTS)
        def _():
            part_copy(i, True).wait()
        act_copy(1, i).wait_recv()

        @pl.when(i < CHUNKS - AHEAD)
        def _():
            act_copy(1, i + AHEAD).start()

        @pl.when(i == CHUNKS - AHEAD)
        def _():
            w_copy(1, 6).start()
            w_copy(1, 8).start()

        @pl.when(i == CHUNKS - 2)
        def _():
            dw2_dep().wait()
            dw2t[:, dw2_mine] += dw2t[:, dw2_landing]
            dw2_out().start()

        @pl.when(i == CHUNKS - 1)
        def _():
            dw2_out().wait()
            for peer in (sibling, layer):
                pl.semaphore_signal(free_sem, inc=1, device_id=peer, device_id_type=MESH)

        acc[slot] = jnp.zeros_like(acc[slot])

        @pl.loop(0, hf)
        def _(jj):
            rows, du = backward(i, jj, i * hf + jj, slot)
            dw1[:, pl.ds(al(jj * f, f), f)] += dot(xf[rows, :], du, 0, 0)

            @pl.when(i == CHUNKS - 1)
            def _():
                @pl.when(jj == 0)
                def _():
                    pl.semaphore_wait(free_sem, 2)
                dw1_row(jj).start()

                @pl.when(jj >= 2)
                def _():
                    dw1_take(jj - 2)
                    dw1_dep(jj - 2).start()

        part_copy(i, True).start()

    dw1_take(hf - 2)
    dw1_dep(hf - 2).start()
    dw1_take(hf - 1)
    dw1_dep(hf - 1, f - e).start()
    dw1_give().start()
    for i in (0, 1):
        part_copy(i, True).wait()
        part_copy(i, False).start()
    slope_in(CHUNKS * hf + RING - 1).start()
    w_copy(1, 6).wait_recv()
    w_copy(1, 7).start()
    w_copy(1, 7).wait_recv()

    @pl.loop(0, 2 * CHUNKS)
    def _(k):
        last = k // CHUNKS
        i = lax.rem(k, CHUNKS)
        slot = lax.rem(k, SLOTS)
        part_copy(k, False).wait()

        @pl.when(k < CHUNKS + 2)
        def _():
            part_copy(k + 2, True).wait()

        @pl.when(k < 2 * CHUNKS - 2)
        def _():
            part_copy(k + 2, False).start()

        @pl.when(k == CHUNKS)
        def _():
            w_copy(1, 8).wait_recv()
            w_copy(1, 9).start()
            w_copy(1, 9).wait_recv()

        m = CHUNKS * hf + 2 * k
        slope_in(m).wait()
        slope_in(m + 1).wait()
        rows = pl.ds(al(i * t, t), t)
        for b in range(2):
            cols = pl.ds(al(block_of(hf + 2 * last + b) * f, f), f)
            da = dot(gf[rows, :], w2[cols, :], 1, 1)
            du = (da * ring[lax.rem(m + b, RING)]).astype(BF16)
            acc[slot] += dot(du, w1[own_cols, cols], 1, 1)

        @pl.when(k < 2 * CHUNKS - 2)
        def _():
            slope_in(m + 4).start()
            slope_in(m + 5).start()

        @pl.when(last == 0)
        def _():
            part_copy(k, True).start()

        @pl.when(last == 1)
        def _():
            @pl.when(i >= 1)
            def _():
                put(dx_hbm, i).wait()
            out_buf[...] = acc[slot].astype(BF16)
            put(dx_hbm, i).start()

    for what in (0, 1, 2, 3, 4):
        for k in range(2):
            w_copy(k, what).wait_send()
    for what in (6, 7, 8, 9):
        w_copy(1, what).wait_send()
    for k in range(2):
        for i in range(CHUNKS):
            act_copy(k, i).wait_send()
    put(dx_hbm, 0).wait()
    for b in range(hf):
        w = f if b < hf - 1 else f - e
        dw1_dep(b, w).wait_recv()
        dw1[pl.ds(al(r * half + d * q, q), q), b * f:b * f + w] += dw2t[0:q, hcols + b * f:hcols + b * f + w]
        dw1_out(b).start()
    for b in range(hf):
        dw1_row(b).wait_send()
        dw1_out(b).wait()
        dw1_dep(b, f if b < hf - 1 else f - e).wait_send()
    dw1_give().wait()


def finish_kernel(y_in, dx_in, dw1_in, dw2_in, y_out, dx_out, dw1_out, dw2_out, y, dx, dw1, dw2t, dw2, in_sem, out_sem):
    copies = []
    for src, buf, dst, n in ((y_in, y, y_out, PIECES), (dw2_in, dw2t, None, PIECES), (dx_in, dx, dx_out, PIECES), (dw1_in, dw1, dw1_out, PIECES // 2)):
        rows = src.shape[0] // n
        for p in range(n):
            sl = pl.ds(p * rows, rows)
            copies.append((src.at[sl, :], buf.at[sl, :], None if dst is None else dst.at[sl, :]))
    ins = [pltpu.make_async_copy(a, b, in_sem.at[k]) for k, (a, b, _) in enumerate(copies)]
    for cp in ins:
        cp.start()
    outs = []
    for k, (_, b, o) in enumerate(copies):
        ins[k].wait()
        if o is None:
            rows = dw2t.shape[0] // PIECES
            p = k - PIECES
            dw2[:, p * rows:(p + 1) * rows] = dw2t[p * rows:(p + 1) * rows, :].T
            if p == PIECES - 1:
                outs.append(pltpu.make_async_copy(dw2, dw2_out, out_sem.at[k]))
                outs[-1].start()
        else:
            outs.append(pltpu.make_async_copy(b, o, out_sem.at[k]))
            outs[-1].start()
    for cp in outs:
        cp.wait()


def finish(y, dx, dw1, dw2t):
    sds = jax.ShapeDtypeStruct
    n = 3 * PIECES + PIECES // 2
    return pl.pallas_call(
        finish_kernel,
        out_shape=[sds(y.shape, BF16), sds(dx.shape, BF16), sds(dw1.shape, F32), sds(dw2t.shape[::-1], F32)],
        in_specs=[pl.BlockSpec(memory_space=pl.ANY)] * 4,
        out_specs=[pl.BlockSpec(memory_space=pl.ANY)] * 4,
        scratch_shapes=[
            pltpu.VMEM(y.shape, BF16), pltpu.VMEM(dx.shape, BF16), pltpu.VMEM(dw1.shape, F32),
            pltpu.VMEM(dw2t.shape, F32), pltpu.VMEM(dw2t.shape[::-1], F32),
            pltpu.SemaphoreType.DMA((n,)), pltpu.SemaphoreType.DMA((n,)),
        ],
        compiler_params=pltpu.CompilerParams(vmem_limit_bytes=60 * 1024 * 1024),
        cost_estimate=pl.CostEstimate(flops=2 * 10 ** 9, bytes_accessed=24 * 2 ** 20, transcendentals=0),
        name="finish",
    )(y, dx, dw1, dw2t)


def solution(mesh):
    act_spec = P(("dep", "row"), "col")
    wgt_spec = P("row", "col")
    grad_spec = P(("row", "dep"), "col")

    def local_block(x, w1, w2, g):
        tokens, half = x.shape
        hidden, hcols = w1.shape[0] * 2, w1.shape[1]
        ffn = hcols * 2
        t, f = tokens // CHUNKS, ffn // BLOCKS
        sds = jax.ShapeDtypeStruct
        dma = pltpu.SemaphoreType.DMA
        outs = pl.pallas_call(
            kernel,
            out_shape=[
                sds((tokens, half), BF16), sds((tokens, half), BF16),
                sds((half // 2, hcols), F32),
                sds((half, ffn // 4), F32),
                sds((half // 2, f // 2), F32), sds((CHUNKS, BLOCKS, t, f), F32), sds((CHUNKS, t, half), F32),
            ],
            in_specs=[pl.BlockSpec(memory_space=pl.ANY)] * 4,
            out_specs=[pl.BlockSpec(memory_space=pl.ANY)] * 7,
            scratch_shapes=[
                pltpu.VMEM((hidden, ffn), BF16), pltpu.VMEM((ffn, hidden), BF16),
                pltpu.VMEM((tokens, hidden), BF16), pltpu.VMEM((tokens, hidden), BF16),
                pltpu.VMEM((hidden, hcols), F32), pltpu.VMEM((half, ffn), F32),
                pltpu.VMEM((RING, t, f), F32), pltpu.VMEM((SLOTS, t, half), F32), pltpu.VMEM((t, half), BF16),
                dma((4,)), dma((2, 10)), dma((2, 10)), dma((2, CHUNKS)), dma((2, CHUNKS)),
                dma((RING,)), dma((SLOTS,)), dma((1,)),
                dma((1 + BLOCKS // 2,)), dma((1 + BLOCKS // 2,)), dma((1 + BLOCKS // 2,)), dma((1 + BLOCKS // 2,)), dma((1 + BLOCKS // 2,)), dma((1,)),
                pltpu.SemaphoreType.REGULAR, pltpu.SemaphoreType.REGULAR,
            ],
            compiler_params=pltpu.CompilerParams(collective_id=0, has_side_effects=True, vmem_limit_bytes=67043328),
            name="mlp_block",
        )(x, w1, w2, g)
        got = lax.ppermute(outs[4], "dep", [(0, 1), (1, 0)])
        y, dx, dw1, dw2 = finish(*outs[:4])
        return y, dx, dw1.at[:, hcols - f // 2:].add(got), dw2

    return jax.shard_map(local_block, mesh=mesh, in_specs=(act_spec, wgt_spec, wgt_spec, act_spec), out_specs=(act_spec, act_spec, grad_spec, grad_spec), check_vma=False)
```

```python
import functools

import jax
import jax.numpy as jnp
from jax import lax
from jax.experimental import pallas as pl
from jax.experimental.pallas import tpu as pltpu
from jax.sharding import PartitionSpec as P

GELU_COEF = 0.7978845608028654
CUBIC_COEF = 0.044715
MESH = pl.DeviceIdType.MESH
F32, BF16 = jnp.float32, jnp.bfloat16
CHUNKS = 8
BLOCKS = 8
RING = 4
AHEAD = 4
SLOTS = 4
PIECES = 4


def gelu_and_slope(u):
    u2 = u * u
    p = GELU_COEF * CUBIC_COEF * u2 + GELU_COEF
    s = 0.5 * jnp.tanh(u * p) + 0.5
    a = u * s
    return a, s + (a * (1.0 - s)) * (6.0 * GELU_COEF * CUBIC_COEF * u2 + 2.0 * GELU_COEF)


def dot(a, b, ca=1, cb=0):
    return lax.dot_general(a, b, (((ca,), (cb,)), ((), ())), preferred_element_type=F32)


def kernel(x_hbm, w1_hbm, w2_hbm, g_hbm, y_hbm, dx_hbm, dw1_own, dw2_own, give_hbm, slope_hbm, part_hbm,
           w1, w2, xf, gf, dw1, dw2t, ring, acc, out_buf,
           load_sem, w_send, w_recv, x_send, x_recv, ring_sem, acc_sem, out_sem, row_send, row_recv, dep_send, dep_recv, own_sem, give_sem, free_sem, room_sem):
    d, c, r = lax.axis_index("dep"), lax.axis_index("col"), lax.axis_index("row")
    o = 1 - c
    across, layer, sibling = (d, o, r), (1 - d, c, r), (d, c, 1 - r)
    tokens, half = x_hbm.shape
    t = tokens // CHUNKS
    ffn = w1.shape[1]
    f = ffn // BLOCKS
    hf = BLOCKS // 2
    hcols, qcols, q = ffn // 2, ffn // 4, half // 2
    e = f // 2

    barrier = pltpu.get_barrier_semaphore()
    for peer in (across, layer, sibling):
        pl.semaphore_signal(barrier, inc=1, device_id=peer, device_id_type=MESH)
    pl.semaphore_wait(barrier, 3)

    def remote(src, dst, send, recv, dev):
        return pltpu.make_async_remote_copy(src_ref=src, dst_ref=dst, send_sem=send, recv_sem=recv, device_id=dev, device_id_type=MESH)

    def al(v, m):
        return pl.multiple_of(v, m)

    wts = ((w1_hbm, w1), (w2_hbm, w2))

    def w_copy(k, what):
        hbm, ref = wts[k]
        rows, cols = hbm.shape

        def span(start, size, col):
            return ref.at[pl.ds(al(start, size), size), pl.ds(al(col * cols, cols), cols)]

        def part(dep, col):
            if k == 0:
                return span(r * rows + dep * (rows // 2), rows // 2, col)
            return span((1 - col) * rows + dep * (rows // 2) + r * (rows // 4), rows // 4, col)

        def late(col):
            if what >= 10:
                return span(col * rows + rows // 2 + r * (rows // 4), rows // 4, col)
            return span(col * rows + (what // 8) * (rows // 4) + r * (rows // 8), rows // 8, col)

        block = span(r * rows, rows, c)
        if what == 5:
            return pltpu.make_async_copy(hbm, block, load_sem.at[k])
        if what >= 6:
            src, dst, dev = (late(c), late(c), across) if what % 2 == 0 else (late(o), late(o), sibling)
        else:
            src, dst, dev = (
                (hbm.at[pl.ds(al(d * (rows // 2), rows // 2), rows // 2), :] if k == 0 else part(d, c), part(d, c), across),
                (hbm, block, sibling),
                (part(d, o), part(d, o), layer),
                (part(d, o), part(d, o), sibling),
                (part(1 - d, o), part(1 - d, o), sibling),
            )[what]
        return remote(src, dst, w_send.at[k, what], w_recv.at[k, what], dev)

    acts = ((x_hbm, xf), (g_hbm, gf))

    def act_copy(k, i):
        hbm, ref = acts[k]
        rows = pl.ds(al(i * t, t), t)
        return remote(hbm.at[rows, :], ref.at[rows, pl.ds(al(c * half, half), half)], x_send.at[k, i], x_recv.at[k, i], across)

    def act_load(k):
        hbm, ref = acts[k]
        return pltpu.make_async_copy(hbm, ref.at[:, pl.ds(al(c * half, half), half)], load_sem.at[2 + k])

    w_copy(0, 0).start()
    act_copy(0, 0).start()
    for k in range(2):
        w_copy(k, 5).start()
        w_copy(k, 1).start()
    for k in range(2):
        act_load(k).start()
    dw2t[...] = jnp.zeros_like(dw2t)
    w_copy(0, 0).wait_recv()
    w_copy(0, 2).start()
    w_copy(0, 3).start()
    for i in range(1, AHEAD):
        act_copy(0, i).start()
    for k in range(2):
        w_copy(k, 5).wait()
        w_copy(k, 1).wait_recv()
        act_load(k).wait()

    def block_of(jj):
        return lax.rem(c * hf + jj, BLOCKS)

    def slope_out(i, jj, slot):
        return pltpu.make_async_copy(ring.at[slot], slope_hbm.at[i, jj], ring_sem.at[slot])

    def slope_in(m):
        first = CHUNKS * hf
        n = jnp.maximum(m - first, 0)
        i = jnp.where(n < 2 * SLOTS, lax.rem(n, SLOTS), lax.rem(n, first // 2) // 2)
        jj = hf + jnp.where(n < 2 * SLOTS, n // SLOTS, (n // (first // 2)) * 2 + lax.rem(n, 2))
        i = jnp.where(m < first, m // hf, i)
        jj = jnp.where(m < first, lax.rem(m, hf), jj)
        slot = lax.rem(m, RING)
        return pltpu.make_async_copy(slope_hbm.at[i, jj], ring.at[slot], ring_sem.at[slot])

    def put(ref, i):
        return pltpu.make_async_copy(out_buf, ref.at[pl.ds(al(i * t, t), t), :], out_sem.at[0])

    own_cols = pl.ds(al(c * half, half), half)

    @pl.loop(0, CHUNKS)
    def _(i):
        rows = pl.ds(al(i * t, t), t)
        act_copy(0, i).wait_recv()

        @pl.when(i < CHUNKS - AHEAD)
        def _():
            act_copy(0, i + AHEAD).start()

        @pl.when(i == CHUNKS - AHEAD)
        def _():
            w_copy(1, 0).start()

        @pl.when(i >= CHUNKS - AHEAD)
        def _():
            act_copy(1, i + AHEAD - CHUNKS).start()

        acc[0] = jnp.zeros_like(acc[0])

        @pl.loop(0, BLOCKS)
        def _(jj):
            n = i * BLOCKS + jj
            slot = lax.rem(n, RING)
            cols = pl.ds(al(block_of(jj) * f, f), f)

            @pl.when(n >= RING)
            def _():
                slope_out(i, jj, slot).wait()

            @pl.when(n == hf)
            def _():
                w_copy(0, 2).wait_recv()
                w_copy(0, 4).start()
                w_copy(0, 3).wait_recv()
                w_copy(0, 4).wait_recv()

            u = dot(xf[rows, :], w1[:, cols])
            a, slope = gelu_and_slope(u)
            ring[slot] = slope
            a = a.astype(BF16)
            acc[0] += dot(a, w2[cols, own_cols])
            dw2t[:, cols] += dot(gf[rows, own_cols], a, 0, 0)
            slope_out(i, jj, slot).start()

        @pl.when(i >= 1)
        def _():
            put(y_hbm, i).wait()
        out_buf[...] = acc[0].astype(BF16)
        put(y_hbm, i).start()

    other_r = pl.ds(al((1 - r) * hcols, hcols), hcols)
    mine_r = pl.ds(al(r * hcols, hcols), hcols)
    landing = dw1.at[0:half, :]

    def dw2_row():
        return remote(dw2t.at[:, other_r], landing, row_send.at[0], row_recv.at[0], sibling)

    dw2_landing = pl.ds(al((1 - r) * hcols, hcols), qcols)
    dw2_mine = pl.ds(al(r * hcols + d * qcols, qcols), qcols)

    def dw2_dep():
        return remote(dw2t.at[:, pl.ds(al(r * hcols + (1 - d) * qcols, qcols), qcols)], dw2t.at[:, dw2_landing], dep_send.at[0], dep_recv.at[0], layer)

    def dw2_out():
        return pltpu.make_async_copy(dw2t.at[:, dw2_mine], dw2_own, own_sem.at[0])

    dw2_row().start()
    for s in range(RING):
        slope_out(0, 0, s).wait()
    for m in range(RING - 1):
        slope_in(m).start()
    put(y_hbm, 0).wait()

    w_copy(1, 0).wait_recv()
    w_copy(1, 2).start()
    w_copy(1, 3).start()
    dw2_row().wait()
    pl.semaphore_signal(room_sem, inc=1, device_id=layer, device_id_type=MESH)
    dw2t[:, mine_r] += landing[...]
    pl.semaphore_wait(room_sem, 1)
    dw2_dep().start()
    dw1[...] = jnp.zeros_like(dw1)

    w_copy(1, 2).wait_recv()
    w_copy(1, 4).start()
    w_copy(1, 3).wait_recv()
    w_copy(1, 4).wait_recv()

    def backward(i, jj, m, slot):
        rows = pl.ds(al(i * t, t), t)
        cols = pl.ds(al(block_of(jj) * f, f), f)
        slope_in(m).wait()
        slope_in(m + RING - 1).start()
        da = dot(gf[rows, :], w2[cols, :], 1, 1)
        du = (da * ring[lax.rem(m, RING)]).astype(BF16)
        acc[slot] += dot(du, w1[own_cols, cols], 1, 1)
        return rows, du

    def part_copy(i, out):
        far, near, sem = part_hbm.at[lax.rem(i, CHUNKS)], acc.at[lax.rem(i, SLOTS)], acc_sem.at[lax.rem(i, SLOTS)]
        return pltpu.make_async_copy(near, far, sem) if out else pltpu.make_async_copy(far, near, sem)

    def dw1_row(b, own):
        cols = pl.ds(al(b * f, f), f)
        part = q * lax.rem(own + 1 + d, 2)
        src = dw1.at[pl.ds(al((1 - r) * half + part, q), q), cols]
        n = 1 + b + own * hf
        return remote(src, dw2t.at[pl.ds(al(part, q), q), cols], row_send.at[n], row_recv.at[n], sibling)

    def dw1_dep(b, width=f):
        src = dw1.at[pl.ds(al(r * half + (1 - d) * q, q), q), pl.ds(al(b * f, f), width)]
        dst = dw2t.at[0:q, pl.ds(al(hcols + b * f, f), width)]
        return remote(src, dst, dep_send.at[1 + b], dep_recv.at[1 + b], layer)

    def dw1_out(b):
        cols = pl.ds(al(b * f, f), f)
        return pltpu.make_async_copy(dw1.at[pl.ds(al(r * half + d * q, q), q), cols], dw1_own.at[:, cols], own_sem.at[1 + b])

    def dw1_take(b, own):
        cols = pl.ds(al(b * f, f), f)
        part = q * lax.rem(own + 1 + d, 2)
        dw1_row(b, own).wait_recv()
        dw1[pl.ds(al(r * half + part, q), q), cols] += dw2t[pl.ds(al(part, q), q), cols]

    def dw1_give():
        return pltpu.make_async_copy(dw1.at[pl.ds(al(r * half + (1 - d) * q, q), q), pl.ds(hcols - e, e)], give_hbm, give_sem.at[0])

    @pl.loop(0, CHUNKS)
    def _(i):
        slot = lax.rem(i, SLOTS)

        @pl.when(i >= SLOTS)
        def _():
            part_copy(i, True).wait()
        act_copy(1, i).wait_recv()

        @pl.when(i < CHUNKS - AHEAD)
        def _():
            act_copy(1, i + AHEAD).start()

        @pl.when(i == CHUNKS - AHEAD)
        def _():
            w_copy(1, 6).start()
            w_copy(1, 8).start()
            w_copy(1, 10).start()

        @pl.when(i == CHUNKS - 2)
        def _():
            dw2_dep().wait()
            dw2t[:, dw2_mine] += dw2t[:, dw2_landing]
            dw2_out().start()

        @pl.when(i == CHUNKS - 1)
        def _():
            dw2_out().wait()
            for peer in (sibling, layer):
                pl.semaphore_signal(free_sem, inc=1, device_id=peer, device_id_type=MESH)

        acc[slot] = jnp.zeros_like(acc[slot])

        @pl.loop(0, hf)
        def _(jj):
            rows, du = backward(i, jj, i * hf + jj, slot)
            dw1[:, pl.ds(al(jj * f, f), f)] += dot(xf[rows, :], du, 0, 0)

            @pl.when(i == CHUNKS - 1)
            def _():
                @pl.when(jj == 0)
                def _():
                    pl.semaphore_wait(free_sem, 2)
                dw1_row(jj, 0).start()
                dw1_row(jj, 1).start()

                @pl.when(lax.rem(jj, 2) == 1)
                def _():
                    dw1_take(jj // 2, 0)
                    dw1_dep(jj // 2).start()

        part_copy(i, True).start()

    for b in range(hf // 2, hf):
        dw1_take(b, 0)
        dw1_dep(b, f if b < hf - 1 else f - e).start()
    dw1_give().start()
    for b in range(hf):
        dw1_take(b, 1)
    for i in range(SLOTS):
        part_copy(i, True).wait()
        part_copy(i, False).start()
    slope_in(CHUNKS * hf + RING - 1).start()

    def late_piece(what):
        w_copy(1, what).wait_recv()
        w_copy(1, what + 1).start()
        w_copy(1, what + 1).wait_recv()

    def second_pass(i, jj, count, m, slot):
        for b in range(count):
            slope_in(m + b).wait()
        rows = pl.ds(al(i * t, t), t)
        for b in range(count):
            cols = pl.ds(al(block_of(jj + b) * f, f), f)
            da = dot(gf[rows, :], w2[cols, :], 1, 1)
            du = (da * ring[lax.rem(m + b, RING)]).astype(BF16)
            acc[slot] += dot(du, w1[own_cols, cols], 1, 1)

    late_piece(6)

    @pl.loop(0, SLOTS)
    def _(k):
        part_copy(k, False).wait()
        second_pass(k, hf, 1, CHUNKS * hf + k, k)
        slope_in(CHUNKS * hf + k + RING).start()

    late_piece(8)

    @pl.loop(0, SLOTS)
    def _(k):
        @pl.when(k >= 2)
        def _():
            part_copy(k + 2, True).wait()
            part_copy(k + 2, False).start()
        second_pass(k, hf + 1, 1, CHUNKS * hf + SLOTS + k, k)
        slope_in(CHUNKS * hf + SLOTS + k + RING).start()
        part_copy(k, True).start()

    @pl.loop(SLOTS, 2 * CHUNKS)
    def _(k):
        last = k // CHUNKS
        i = lax.rem(k, CHUNKS)
        slot = lax.rem(k, SLOTS)
        part_copy(k, False).wait()

        @pl.when(k < CHUNKS + 2)
        def _():
            part_copy(k + 2, True).wait()

        @pl.when(k < 2 * CHUNKS - 2)
        def _():
            part_copy(k + 2, False).start()

        @pl.when(k == CHUNKS)
        def _():
            late_piece(10)

        m = CHUNKS * hf + 2 * k
        second_pass(i, hf + 2 * last, 2, m, slot)

        @pl.when(k < 2 * CHUNKS - 2)
        def _():
            slope_in(m + 4).start()
            slope_in(m + 5).start()

        @pl.when(last == 0)
        def _():
            part_copy(k, True).start()

        @pl.when(last == 1)
        def _():
            @pl.when(i >= 1)
            def _():
                put(dx_hbm, i).wait()
            out_buf[...] = acc[slot].astype(BF16)
            put(dx_hbm, i).start()

    for what in (0, 1, 2, 3, 4):
        for k in range(2):
            w_copy(k, what).wait_send()
    for what in range(6, 12):
        w_copy(1, what).wait_send()
    for k in range(2):
        for i in range(CHUNKS):
            act_copy(k, i).wait_send()
    put(dx_hbm, 0).wait()
    for b in range(hf):
        w = f if b < hf - 1 else f - e
        dw1_dep(b, w).wait_recv()
        dw1[pl.ds(al(r * half + d * q, q), q), b * f:b * f + w] += dw2t[0:q, hcols + b * f:hcols + b * f + w]
        dw1_out(b).start()
    for b in range(hf):
        dw1_row(b, 0).wait_send()
        dw1_row(b, 1).wait_send()
        dw1_out(b).wait()
        dw1_dep(b, f if b < hf - 1 else f - e).wait_send()
    dw1_give().wait()


def finish_kernel(y_in, dx_in, dw1_in, dw2_in, y_out, dx_out, dw1_out, dw2_out, y, dx, dw1, dw2t, dw2, in_sem, out_sem):
    copies = []
    for src, buf, dst, n in ((y_in, y, y_out, PIECES), (dw2_in, dw2t, None, PIECES), (dx_in, dx, dx_out, PIECES), (dw1_in, dw1, dw1_out, PIECES // 2)):
        rows = src.shape[0] // n
        for p in range(n):
            sl = pl.ds(p * rows, rows)
            copies.append((src.at[sl, :], buf.at[sl, :], None if dst is None else dst.at[sl, :]))
    ins = [pltpu.make_async_copy(a, b, in_sem.at[k]) for k, (a, b, _) in enumerate(copies)]
    for cp in ins:
        cp.start()
    outs = []
    for k, (_, b, o) in enumerate(copies):
        ins[k].wait()
        if o is None:
            rows = dw2t.shape[0] // PIECES
            p = k - PIECES
            dw2[:, p * rows:(p + 1) * rows] = dw2t[p * rows:(p + 1) * rows, :].T
            if p == PIECES - 1:
                outs.append(pltpu.make_async_copy(dw2, dw2_out, out_sem.at[k]))
                outs[-1].start()
        else:
            outs.append(pltpu.make_async_copy(b, o, out_sem.at[k]))
            outs[-1].start()
    for cp in outs:
        cp.wait()


def finish(y, dx, dw1, dw2t):
    sds = jax.ShapeDtypeStruct
    n = 3 * PIECES + PIECES // 2
    return pl.pallas_call(
        finish_kernel,
        out_shape=[sds(y.shape, BF16), sds(dx.shape, BF16), sds(dw1.shape, F32), sds(dw2t.shape[::-1], F32)],
        in_specs=[pl.BlockSpec(memory_space=pl.ANY)] * 4,
        out_specs=[pl.BlockSpec(memory_space=pl.ANY)] * 4,
        scratch_shapes=[
            pltpu.VMEM(y.shape, BF16), pltpu.VMEM(dx.shape, BF16), pltpu.VMEM(dw1.shape, F32),
            pltpu.VMEM(dw2t.shape, F32), pltpu.VMEM(dw2t.shape[::-1], F32),
            pltpu.SemaphoreType.DMA((n,)), pltpu.SemaphoreType.DMA((n,)),
        ],
        compiler_params=pltpu.CompilerParams(vmem_limit_bytes=60 * 1024 * 1024),
        cost_estimate=pl.CostEstimate(flops=2 * 10 ** 9, bytes_accessed=24 * 2 ** 20, transcendentals=0),
        name="finish",
    )(y, dx, dw1, dw2t)


def solution(mesh):
    act_spec = P(("dep", "row"), "col")
    wgt_spec = P("row", "col")
    grad_spec = P(("row", "dep"), "col")

    def local_block(x, w1, w2, g):
        tokens, half = x.shape
        hidden, hcols = w1.shape[0] * 2, w1.shape[1]
        ffn = hcols * 2
        t, f = tokens // CHUNKS, ffn // BLOCKS
        sds = jax.ShapeDtypeStruct
        dma = pltpu.SemaphoreType.DMA
        outs = pl.pallas_call(
            kernel,
            out_shape=[
                sds((tokens, half), BF16), sds((tokens, half), BF16),
                sds((half // 2, hcols), F32),
                sds((half, ffn // 4), F32),
                sds((half // 2, f // 2), F32), sds((CHUNKS, BLOCKS, t, f), F32), sds((CHUNKS, t, half), F32),
            ],
            in_specs=[pl.BlockSpec(memory_space=pl.ANY)] * 4,
            out_specs=[pl.BlockSpec(memory_space=pl.ANY)] * 7,
            scratch_shapes=[
                pltpu.VMEM((hidden, ffn), BF16), pltpu.VMEM((ffn, hidden), BF16),
                pltpu.VMEM((tokens, hidden), BF16), pltpu.VMEM((tokens, hidden), BF16),
                pltpu.VMEM((hidden, hcols), F32), pltpu.VMEM((half, ffn), F32),
                pltpu.VMEM((RING, t, f), F32), pltpu.VMEM((SLOTS, t, half), F32), pltpu.VMEM((t, half), BF16),
                dma((4,)), dma((2, 12)), dma((2, 12)), dma((2, CHUNKS)), dma((2, CHUNKS)),
                dma((RING,)), dma((SLOTS,)), dma((1,)),
                dma((1 + BLOCKS,)), dma((1 + BLOCKS,)), dma((1 + BLOCKS // 2,)), dma((1 + BLOCKS // 2,)), dma((1 + BLOCKS // 2,)), dma((1,)),
                pltpu.SemaphoreType.REGULAR, pltpu.SemaphoreType.REGULAR,
            ],
            compiler_params=pltpu.CompilerParams(collective_id=0, has_side_effects=True, vmem_limit_bytes=67043328),
            name="mlp_block",
        )(x, w1, w2, g)
        got = lax.ppermute(outs[4], "dep", [(0, 1), (1, 0)])
        y, dx, dw1, dw2 = finish(*outs[:4])
        return y, dx, dw1.at[:, hcols - f // 2:].add(got), dw2

    return jax.shard_map(local_block, mesh=mesh, in_specs=(act_spec, wgt_spec, wgt_spec, act_spec), out_specs=(act_spec, act_spec, grad_spec, grad_spec), check_vma=False)
```
